256 devices in a mesh: client: 16 (over y_lo, z), tensor: 8 (over x, core), sdata: 2 (over y_hi).
Axes of the slice: x: 4, y: 4 (y_hi: 2, y_lo: 2; y = y_hi * 2 + y_lo), z: 8, core: 2. Of those that a mesh axis runs over, the one named last changes fastest.
Arguments:
- client_input: bfloat16 [12288, 2048], P(('client', 'sdata')), may hold values from -6 to 6
- client_gain: bfloat16 [16, 2048], P('client'), may hold values from 0.5 to 1.5
- query_weight: bfloat16 [16, 2048, 2048], P('client', None, 'tensor'), as said below
- key_weight: bfloat16 [16, 2048, 512], P('client', None, 'tensor'), as said below
- client_value_weight: bfloat16 [16, 2048, 512], P('client', None, 'tensor'), may hold values from -0.125 to 0.125
- output_weight: bfloat16 [16, 2048, 2048], P('client', None, 'tensor'), may hold values from -0.125 to 0.125
- server_gain: bfloat16 [2, 2048], P('sdata'), may hold values from 0.5 to 1.5
- server_gate: bfloat16 [2, 2048, 4096], P('sdata', None, 'tensor'), may hold values from -0.125 to 0.125
- server_up: bfloat16 [2, 2048, 4096], P('sdata', None, 'tensor'), may hold values from -0.125 to 0.125
- server_down: bfloat16 [2, 4096, 2048], P('sdata', 'tensor'), may hold values from -0.09375 to 0.09375
- upstream: bfloat16 [12288, 2048], P(('client', 'sdata')), may hold values from -6 to 6
- assignment: int32 [16], replicated, may hold values from 0 to 1, as said below
Outputs:
- query_update: bfloat16 [2048, 2048], P(('client', 'sdata'), 'tensor')
- key_update: bfloat16 [2048, 512], P(('client', 'sdata'), 'tensor')
- value_update: bfloat16 [2048, 512], P(('client', 'sdata'), 'tensor')
- output_update: bfloat16 [2048, 2048], P(('client', 'sdata'), 'tensor')
The draws below stay inside these ranges and needn't reach their ends.
Inputs may be any that keep to these rules, and one draw needn't show every extreme that they name: `assignment`: each of the 2 server groups is named by exactly 8 clients. `query_weight`: independent entries with a spread of about 2048 ** -0.5. `key_weight`: entries with a spread of about 2048 ** -0.5 or more.
All inputs are finite; a program needn't handle non-finite values.
Results may differ from the reference program's by a relative error of at most 0.038.
The reference program's roundings to bfloat16 on the way count: a program that leaves them out, or rounds other values in their place, can miss the bound.
Values may be sent and summed in bfloat16 or wider, within the bound.
No kernel may reach another device: no remote copies, remote signals or barrier semaphores. Data moves between devices by JAX's collectives and lax.ppermute only.
A program may use at most 128 MiB of HBM per device.

```python
import math
import jax
import jax.numpy as jnp
from jax import lax

MODEL_WIDTH = 2048
HEAD_DIM = 64
FF = 4096
LEN = 384
CLIENT_TOTAL = 16
GROUPS = 2
TOKENS = 12288
QUERY_FEATURES = 2048
KEY_FEATURES = 512


def weights_pair(key):
    scaling_factor = MODEL_WIDTH ** (-0.5)
    query_matrix = jnp.clip(jax.random.normal(jax.random.fold_in(key, 11), (CLIENT_TOTAL, MODEL_WIDTH, QUERY_FEATURES), jnp.float32), -4.0, 4.0) * scaling_factor
    client_key_matrix = jnp.clip(jax.random.normal(jax.random.fold_in(key, 12), (CLIENT_TOTAL, MODEL_WIDTH, KEY_FEATURES), jnp.float32), -4.0, 4.0) * scaling_factor
    return (query_matrix, client_key_matrix)


def draw_query_weight(key, part):
    return weights_pair(key)[0].astype(jnp.bfloat16)


def draw_key_weight(key, part):
    return weights_pair(key)[1].astype(jnp.bfloat16)


def draw_assignment(key, part):
    scores = jax.random.randint(jax.random.fold_in(key, 4099), (CLIENT_TOTAL,), 0, 1 << 20) * CLIENT_TOTAL + jnp.arange(CLIENT_TOTAL)
    order = jnp.argsort(scores, stable=True)
    return (order % GROUPS).astype(jnp.int32)


def strengthened(entries, own_key, source, target, shards_of, factor):
    def block_of(axis_at):
        return (jnp.arange(entries.shape[axis_at]) // (entries.shape[axis_at] // shards_of)).reshape((-1,) + (1,) * (entries.ndim - 1 - axis_at))

    near = jax.random.permutation(own_key, shards_of)[block_of(target)]
    far = (block_of(target) + shards_of // 2) % shards_of
    return jnp.where((block_of(source) == near) | (block_of(source) == far), factor * entries, entries)


def level_of(key, shape, pieces, least, largest):
    def one(dim, parts):
        steps = jax.random.uniform(jax.random.fold_in(jax.random.fold_in(key, 6), dim), (parts,), jnp.float32, least / len(pieces), largest / len(pieces))
        return jnp.repeat(jnp.exp(steps), shape[dim] // parts).reshape((-1,) + (1,) * (len(shape) - dim - 1))

    level = one(*pieces[0])
    for cut in pieces[1:]:
        level = level * one(*cut)
    return level


def noise(rng, shape, deviation, most, pieces=(), kind=jnp.bfloat16):
    array = jax.random.normal(rng, shape, jnp.float32) * deviation
    if len(pieces) > 0:
        array = level_of(rng, shape, pieces, -0.22, 0.18) * array
    return jnp.clip(array, min=-most, max=most).astype(kind)


def noise_with(stream_key, shape, scale, limit, pieces, heavy, held_as=jnp.bfloat16):
    array = scale * jax.random.normal(stream_key, shape, jnp.float32)
    if pieces:
        array = array * level_of(stream_key, shape, pieces, -0.22, 0.18)
    return jnp.clip(strengthened(array, jax.random.fold_in(stream_key, 3), *heavy), -limit, limit).astype(held_as)


def setup_inputs(seed: int = 0) -> dict:
    streams_of = jax.random.split(jax.random.key(seed), 13)
    return {
        "client_input": noise_with(streams_of[0], (TOKENS, MODEL_WIDTH), 1.0, 6.0, ((0, 32),), (0, 1, 32, 2.75)),
        "client_gain": jnp.clip(1.0 + 0.1 * jax.random.normal(streams_of[1], (CLIENT_TOTAL, MODEL_WIDTH), jnp.float32), 0.5, 1.5).astype(jnp.bfloat16),
        "query_weight": draw_query_weight(jax.random.fold_in(streams_of[12], 71), 0),
        "key_weight": draw_key_weight(jax.random.fold_in(streams_of[12], 71), 0),
        "client_value_weight": noise(streams_of[4], (CLIENT_TOTAL, MODEL_WIDTH, KEY_FEATURES), MODEL_WIDTH ** -0.5, 0.125, ((0, 16), (2, 8))),
        "output_weight": noise(streams_of[5], (CLIENT_TOTAL, MODEL_WIDTH, QUERY_FEATURES), QUERY_FEATURES ** -0.5, 0.125, ((0, 16), (2, 8))),
        "server_gain": jnp.clip(1.0 + 0.1 * jax.random.normal(streams_of[6], (GROUPS, MODEL_WIDTH), jnp.float32), 0.5, 1.5).astype(jnp.bfloat16),
        "server_gate": noise(streams_of[7], (GROUPS, MODEL_WIDTH, FF), MODEL_WIDTH ** -0.5, 0.125, ((0, 2), (2, 8))),
        "server_up": noise(streams_of[8], (GROUPS, MODEL_WIDTH, FF), MODEL_WIDTH ** -0.5, 0.125, ((0, 2), (2, 8))),
        "server_down": noise(streams_of[9], (GROUPS, FF, MODEL_WIDTH), FF ** -0.5, 0.09375, ((0, 2), (1, 8))),
        "upstream": noise(streams_of[10], (TOKENS, MODEL_WIDTH), 1.0, 6.0, ((0, 32),)),
        "assignment": draw_assignment(jax.random.fold_in(streams_of[12], 71), 0),
    }


def rotary_tables(length):
    halfway = HEAD_DIM // 2
    positions = jnp.arange(length).astype(jnp.float32)
    exponents = jnp.arange(halfway).astype(jnp.float32) * (2.0 / HEAD_DIM)
    frequencies = jnp.exp(-math.log(500000.0) * exponents)
    angles = positions[:, None] * frequencies[None, :]
    cosine_table = jnp.concatenate([jnp.cos(angles), jnp.cos(angles)], 1)
    sine_table = jnp.concatenate([jnp.sin(angles), jnp.sin(angles)], 1)
    return (cosine_table, sine_table)

def rotary(heads_in, cosine_table, sine_table):
    halfway = heads_in.shape[-1] // 2
    turned = jnp.concatenate([-heads_in[..., halfway:], heads_in[..., :halfway]], -1)
    return heads_in * cosine_table[:, None, :] + turned * sine_table[:, None, :]

def normalize(rows_in, gain):
    rows_float = rows_in.astype(jnp.float32)
    inv_rms = lax.rsqrt(lax.optimization_barrier(jnp.mean(rows_float * rows_float, -1, keepdims=True)) + 1e-05)
    return (rows_float * inv_rms * gain.astype(jnp.float32)).astype(jnp.bfloat16)

def attention_part(normed, query_matrix, client_key_matrix, value_matrix, output_matrix):
    length = normed.shape[0]
    query_count = query_matrix.shape[1] // HEAD_DIM
    shared_count = client_key_matrix.shape[1] // HEAD_DIM
    group_size = query_count // shared_count
    cosine_table, sine_table = rotary_tables(length)
    queries = jnp.dot(normed, query_matrix, preferred_element_type=jnp.float32).reshape(length, query_count, HEAD_DIM)
    queries = rotary(queries, cosine_table, sine_table).astype(jnp.bfloat16).reshape(length, shared_count, group_size, HEAD_DIM)
    key_heads = jnp.dot(normed, client_key_matrix, preferred_element_type=jnp.float32).reshape(length, shared_count, HEAD_DIM)
    key_heads = rotary(key_heads, cosine_table, sine_table).astype(jnp.bfloat16)
    value_heads = jnp.dot(normed, value_matrix, preferred_element_type=jnp.float32).astype(jnp.bfloat16).reshape(length, shared_count, HEAD_DIM)
    scores = jnp.einsum('qgrd,kgd->grqk', queries.astype(jnp.float32), key_heads.astype(jnp.float32)) * HEAD_DIM ** (-0.5)
    row_ids = lax.broadcasted_iota(jnp.int32, (length, length), 0)
    col_ids = lax.broadcasted_iota(jnp.int32, (length, length), 1)
    scores = jnp.where(col_ids <= row_ids, scores, -1e+30)
    highest = lax.stop_gradient(lax.optimization_barrier(jnp.max(scores, -1, keepdims=True)))
    exponent = jnp.exp(scores - highest)
    weights = (exponent / lax.optimization_barrier(jnp.sum(exponent, -1, keepdims=True))).astype(jnp.bfloat16)
    context = jnp.einsum('grqk,kgd->qgrd', weights.astype(jnp.float32), value_heads.astype(jnp.float32))
    context = context.astype(jnp.bfloat16).reshape(length, query_count * HEAD_DIM)
    return lax.dot_general(context, output_matrix, (((1,), (1,)), ((), ())), preferred_element_type=jnp.float32)

def server_pull(rows_in, upstream_rows, gain, gate_matrix, up_matrix, down_matrix):
    rows_float = rows_in.astype(jnp.float32)
    inv_rms = lax.rsqrt(lax.optimization_barrier(jnp.mean(rows_float * rows_float, -1, keepdims=True)) + 1e-05)
    gain_float = gain.astype(jnp.float32)
    server_normed = (rows_float * inv_rms * gain_float).astype(jnp.bfloat16)
    gate_value = jnp.dot(server_normed, gate_matrix, preferred_element_type=jnp.float32)
    up_value = jnp.dot(server_normed, up_matrix, preferred_element_type=jnp.float32)
    pulled = lax.dot_general(upstream_rows, down_matrix, (((1,), (1,)), ((), ())), preferred_element_type=jnp.float32)
    sigmoid_gate = jax.nn.sigmoid(gate_value)
    gate_grad = (pulled * up_value * sigmoid_gate * (1.0 + gate_value * (1.0 - sigmoid_gate))).astype(jnp.bfloat16)
    up_grad = (pulled * gate_value * sigmoid_gate).astype(jnp.bfloat16)
    normed_grad = lax.dot_general(gate_grad, gate_matrix, (((1,), (1,)), ((), ())), preferred_element_type=jnp.float32)
    normed_grad = normed_grad + lax.dot_general(up_grad, up_matrix, (((1,), (1,)), ((), ())), preferred_element_type=jnp.float32)
    weighted = normed_grad * gain_float
    return inv_rms * weighted - rows_float * inv_rms ** 3 * lax.optimization_barrier(jnp.mean(weighted * rows_float, -1, keepdims=True))

def reference(client_input, client_gain, query_weight, key_weight, client_value_weight, output_weight, server_gain, server_gate, server_up, server_down, upstream, assignment):
    sequences = client_input.reshape(CLIENT_TOTAL * GROUPS, LEN, MODEL_WIDTH)
    upstream_seqs = upstream.reshape(CLIENT_TOTAL * GROUPS, LEN, MODEL_WIDTH)

    def one_sequence(totals, index_seq):
        owner_client = index_seq // GROUPS
        group_index = assignment[owner_client]
        rows_in = sequences[index_seq]
        upstream_rows = upstream_seqs[index_seq]
        normed = normalize(rows_in, client_gain[owner_client])

        def client_part(query_matrix, client_key_matrix, value_matrix, output_matrix):
            return attention_part(normed, query_matrix, client_key_matrix, value_matrix, output_matrix)
        attended, pullback = jax.vjp(client_part, query_weight[owner_client], key_weight[owner_client], client_value_weight[owner_client], output_weight[owner_client])
        cut_input = (rows_in.astype(jnp.float32) + attended).astype(jnp.bfloat16)
        pulled = server_pull(cut_input, upstream_rows, server_gain[group_index], server_gate[group_index], server_up[group_index], server_down[group_index])
        cut_grad = (upstream_rows.astype(jnp.float32) + pulled).astype(jnp.bfloat16)
        gradients = pullback(cut_grad.astype(jnp.float32))
        updated = tuple((total + grad_item.astype(jnp.bfloat16).astype(jnp.float32) for total, grad_item in zip(totals, gradients)))
        return (updated, None)
    start_offsets = (jnp.zeros((MODEL_WIDTH, QUERY_FEATURES), jnp.float32), jnp.zeros((MODEL_WIDTH, KEY_FEATURES), jnp.float32), jnp.zeros((MODEL_WIDTH, KEY_FEATURES), jnp.float32), jnp.zeros((MODEL_WIDTH, QUERY_FEATURES), jnp.float32))
    totals, unused = lax.scan(one_sequence, start_offsets, jnp.arange(CLIENT_TOTAL * GROUPS).astype(jnp.int32))
    query_total, key_total, value_total, output_total = totals
    return ((query_total / CLIENT_TOTAL).astype(jnp.bfloat16), (key_total / CLIENT_TOTAL).astype(jnp.bfloat16), (value_total / CLIENT_TOTAL).astype(jnp.bfloat16), (output_total / CLIENT_TOTAL).astype(jnp.bfloat16))
```

```python
from functools import partial
import math

import jax
import jax.numpy as jnp
from jax import lax
from jax.sharding import Mesh, PartitionSpec as P

HEAD_DIM = 64


def rotary_tables(length):
    halfway = HEAD_DIM // 2
    positions = jnp.arange(length).astype(jnp.float32)
    exponents = jnp.arange(halfway).astype(jnp.float32) * (2.0 / HEAD_DIM)
    frequencies = jnp.exp(-math.log(500000.0) * exponents)
    angles = positions[:, None] * frequencies[None, :]
    cosine_table = jnp.concatenate([jnp.cos(angles), jnp.cos(angles)], 1)
    sine_table = jnp.concatenate([jnp.sin(angles), jnp.sin(angles)], 1)
    return (cosine_table, sine_table)


def rotary(heads_in, cosine_table, sine_table):
    halfway = heads_in.shape[-1] // 2
    turned = jnp.concatenate([-heads_in[..., halfway:], heads_in[..., :halfway]], -1)
    return heads_in * cosine_table[:, None, :] + turned * sine_table[:, None, :]


def normalize(rows_in, gain):
    rows_float = rows_in.astype(jnp.float32)
    inv_rms = lax.rsqrt(jnp.mean(rows_float * rows_float, -1, keepdims=True) + 1e-05)
    return (rows_float * inv_rms * gain.astype(jnp.float32)).astype(jnp.bfloat16)


def attention_part(normed, query_matrix, client_key_matrix, value_matrix, output_matrix):
    length = normed.shape[0]
    query_count = query_matrix.shape[1] // HEAD_DIM
    shared_count = client_key_matrix.shape[1] // HEAD_DIM
    group_size = query_count // shared_count
    cosine_table, sine_table = rotary_tables(length)
    queries = jnp.dot(normed, query_matrix, preferred_element_type=jnp.float32).reshape(
        length, query_count, HEAD_DIM
    )
    queries = (
        rotary(queries, cosine_table, sine_table)
        .astype(jnp.bfloat16)
        .reshape(length, shared_count, group_size, HEAD_DIM)
    )
    key_heads = jnp.dot(normed, client_key_matrix, preferred_element_type=jnp.float32).reshape(
        length, shared_count, HEAD_DIM
    )
    key_heads = rotary(key_heads, cosine_table, sine_table).astype(jnp.bfloat16)
    value_heads = (
        jnp.dot(normed, value_matrix, preferred_element_type=jnp.float32)
        .astype(jnp.bfloat16)
        .reshape(length, shared_count, HEAD_DIM)
    )
    scores = jnp.einsum(
        "qgrd,kgd->grqk", queries.astype(jnp.float32), key_heads.astype(jnp.float32)
    ) * HEAD_DIM ** (-0.5)
    row_ids = lax.broadcasted_iota(jnp.int32, (length, length), 0)
    col_ids = lax.broadcasted_iota(jnp.int32, (length, length), 1)
    scores = jnp.where(col_ids <= row_ids, scores, -1e30)
    highest = lax.stop_gradient(jnp.max(scores, -1, keepdims=True))
    exponent = jnp.exp(scores - highest)
    weights = (exponent / jnp.sum(exponent, -1, keepdims=True)).astype(jnp.bfloat16)
    context = jnp.einsum(
        "grqk,kgd->qgrd", weights.astype(jnp.float32), value_heads.astype(jnp.float32)
    )
    context = context.astype(jnp.bfloat16).reshape(length, query_count * HEAD_DIM)
    return lax.dot_general(
        context, output_matrix, (((1,), (1,)), ((), ())), preferred_element_type=jnp.float32
    )


def server_pull(rows_in, upstream_rows, gain, gate_matrix, up_matrix, down_matrix):
    rows_float = rows_in.astype(jnp.float32)
    inv_rms = lax.rsqrt(jnp.mean(rows_float * rows_float, -1, keepdims=True) + 1e-05)
    gain_float = gain.astype(jnp.float32)
    server_normed = (rows_float * inv_rms * gain_float).astype(jnp.bfloat16)
    gate_value = jnp.dot(server_normed, gate_matrix, preferred_element_type=jnp.float32)
    up_value = jnp.dot(server_normed, up_matrix, preferred_element_type=jnp.float32)
    pulled = lax.dot_general(
        upstream_rows, down_matrix, (((1,), (1,)), ((), ())), preferred_element_type=jnp.float32
    )
    sigmoid_gate = jax.nn.sigmoid(gate_value)
    gate_grad = (
        pulled * up_value * sigmoid_gate * (1.0 + gate_value * (1.0 - sigmoid_gate))
    ).astype(jnp.bfloat16)
    up_grad = (pulled * gate_value * sigmoid_gate).astype(jnp.bfloat16)
    normed_grad = lax.dot_general(
        gate_grad, gate_matrix, (((1,), (1,)), ((), ())), preferred_element_type=jnp.float32
    )
    normed_grad = normed_grad + lax.dot_general(
        up_grad, up_matrix, (((1,), (1,)), ((), ())), preferred_element_type=jnp.float32
    )
    weighted = normed_grad * gain_float
    return inv_rms * weighted - rows_float * inv_rms**3 * jnp.mean(
        weighted * rows_float, -1, keepdims=True
    )


BLOCK = 256


def x_shift(value, step):
    size = lax.axis_size("x")
    return lax.ppermute(value, "x", [(i, (i + step) % size) for i in range(size)])


def core_swap(value):
    return lax.ppermute(value, "core", [(0, 1), (1, 0)])


def group_swap(value):
    return lax.ppermute(value, "yh", [(0, 1), (1, 0)])


def y_shift(value, step):
    def place(y):
        return (y % 2) * 2 + y // 2

    return lax.ppermute(value, ("yl", "yh"), [(place(y), place((y + step) % 4)) for y in range(4)])


def z_shift(value, step):
    size = lax.axis_size("z")
    return lax.ppermute(value, "z", [(i, (i + step) % size) for i in range(size)])


def over_clients(pieces):
    return lax.all_to_all(pieces, ("yl", "z"), 0, 0, tiled=True)


def relay_out(rows, keep, send):
    pieces = over_clients(rows.reshape(16, -1, BLOCK))
    kept = jnp.take(pieces, keep, axis=0)
    arrived = group_swap(jnp.take(pieces, send, axis=0))
    return jnp.concatenate([kept, arrived], 0).reshape(rows.shape)


def relay_back(rows, inverse):
    pieces = rows.reshape(16, -1, BLOCK)
    returned = group_swap(pieces[8:])
    ordered = jnp.take(jnp.concatenate([pieces[:8], returned], 0), inverse, axis=0)
    return over_clients(ordered).reshape(rows.shape)


def share_sum(partial_rows, x, core):
    blocks = jnp.moveaxis(
        partial_rows.astype(jnp.bfloat16).reshape(partial_rows.shape[0], 8, BLOCK), 1, 0
    )
    turn = (x + jnp.arange(4)) % 4
    mine = jnp.take(blocks, core * 4 + turn, axis=0)
    other = jnp.take(blocks, (1 - core) * 4 + turn, axis=0)
    summed = mine.astype(jnp.float32) + core_swap(other).astype(jnp.float32)
    rounded = summed.astype(jnp.bfloat16)
    parts = [x_shift(rounded[step], step) for step in (1, 3, 2)]
    return summed[0] + sum(part.astype(jnp.float32) for part in parts)


def widen_rows(own, x, core):
    mine = jnp.stack([own] + [x_shift(own, step) for step in (1, 2, 3)])
    other = core_swap(mine)
    both = jnp.concatenate([mine, other], 0)
    block = jnp.arange(8)
    place = ((block // 4 + core) % 2) * 4 + (x - block % 4) % 4
    ordered = jnp.take(both, place, axis=0)
    return jnp.moveaxis(ordered, 0, 1).reshape(own.shape[0], 8 * BLOCK)


def local(
    client_input,
    client_gain,
    query_weight,
    key_weight,
    client_value_weight,
    output_weight,
    server_gain,
    server_gate,
    server_up,
    server_down,
    upstream,
    assignment,
):
    client_count = 16
    x = lax.axis_index("x")
    core = lax.axis_index("core")
    group = lax.axis_index("yh")
    mine_first = (assignment != group).astype(jnp.int32)
    earlier = jnp.arange(16)[:, None] > jnp.arange(16)[None, :]
    same = mine_first[:, None] == mine_first[None, :]
    rank = jnp.sum((earlier & same).astype(jnp.int32), 1)
    inverse = rank + 8 * mine_first
    order = jnp.sum(
        jnp.where(inverse[None, :] == jnp.arange(16)[:, None], jnp.arange(16)[None, :], 0), 1
    )
    keep, send = order[:8], order[8:]
    start = (core * 4 + x) * BLOCK
    own_input = lax.dynamic_slice_in_dim(client_input, start, BLOCK, 1)
    own_upstream = lax.dynamic_slice_in_dim(upstream, start, BLOCK, 1)
    server_upstream = relay_out(own_upstream, keep, send)
    wide_upstream = widen_rows(server_upstream, x, core)
    normed = normalize(client_input, client_gain[0])
    attended, pullback = jax.vjp(
        partial(attention_part, normed),
        query_weight[0],
        key_weight[0],
        client_value_weight[0],
        output_weight[0],
    )
    cut_input = (own_input.astype(jnp.float32) + share_sum(attended, x, core)).astype(jnp.bfloat16)
    server_rows = relay_out(cut_input, keep, send)
    wide_rows = widen_rows(server_rows, x, core)
    pulled = server_pull(
        wide_rows, wide_upstream, server_gain[0], server_gate[0], server_up[0], server_down[0]
    )
    cut_grad = (share_sum(pulled, x, core) + server_upstream.astype(jnp.float32)).astype(
        jnp.bfloat16
    )
    returned = relay_back(cut_grad, inverse)
    arriving_grad = widen_rows(returned, x, core)
    query_grad, key_grad, value_grad, output_grad = pullback(arriving_grad.astype(jnp.float32))
    query_width = query_grad.shape[1]
    key_width = key_grad.shape[1]
    joined = jnp.concatenate([query_grad, key_grad, value_grad, output_grad], 1)
    y = group * 2 + lax.axis_index("yl")
    tiles = joined.reshape(2, 8, 2, 64, -1)

    def for_y(step):
        at = (y + step) % 4
        picked = lax.dynamic_index_in_dim(tiles, at % 2, 0, keepdims=False)
        return lax.dynamic_index_in_dim(picked, at // 2, 1, keepdims=False)

    summed = for_y(0).astype(jnp.float32)
    for step in (1, 3, 2):
        summed = summed + y_shift(for_y(step), step).astype(jnp.float32)
    pieces = lax.all_to_all(summed.astype(jnp.bfloat16), "z", 0, 0, tiled=True)
    total = jnp.sum(pieces.astype(jnp.float32), axis=0) / client_count
    total = total.astype(jnp.bfloat16)
    query_update = total[:, :query_width]
    key_update = total[:, query_width : query_width + key_width]
    value_update = total[:, query_width + key_width : query_width + 2 * key_width]
    output_update = total[:, query_width + 2 * key_width :]
    return (query_update, key_update, value_update, output_update)


def solution(mesh):
    fine = Mesh(mesh.devices.reshape(2, 8, 4, 2, 2), ("yl", "z", "x", "core", "yh"))
    client, tensor, sdata = ("yl", "z"), ("x", "core"), "yh"
    rows = ("yl", "z", "yh")
    placed = (
        P(rows, None),
        P(client, None),
        P(client, None, tensor),
        P(client, None, tensor),
        P(client, None, tensor),
        P(client, None, tensor),
        P(sdata, None),
        P(sdata, None, tensor),
        P(sdata, None, tensor),
        P(sdata, tensor, None),
        P(rows, None),
        P(),
    )
    return jax.shard_map(
        local,
        mesh=fine,
        in_specs=placed,
        out_specs=(P(rows, tensor), P(rows, tensor), P(rows, tensor), P(rows, tensor)),
        check_vma=False,
    )
```

```python
import functools
import math

import jax
import jax.numpy as jnp
from jax import lax
from jax.experimental import pallas as pl
from jax.experimental.pallas import tpu as pltpu
from jax.sharding import Mesh, PartitionSpec as P

HEAD_DIM = 64
HALF = HEAD_DIM // 2
BLOCK = 256
STRIP = 128
F32 = jnp.float32
BF16 = jnp.bfloat16
SMEM = pl.BlockSpec(memory_space=pltpu.SMEM)
VMEM = pl.BlockSpec(memory_space=pltpu.VMEM)


def on_core(kernel, outputs, scratch=()):
    def call(place, *operands):
        return pl.pallas_call(
            kernel,
            out_shape=[jax.ShapeDtypeStruct(shape, kind) for shape, kind in outputs],
            in_specs=[SMEM] + [VMEM] * len(operands),
            out_specs=[VMEM] * len(outputs),
            scratch_shapes=list(scratch),
            compiler_params=pltpu.CompilerParams(vmem_limit_bytes=60 * 1024 * 1024),
        )(place, *operands)

    return call


def dot(a, b):
    return jnp.dot(a, b, preferred_element_type=F32)


def dot_nt(a, b):
    return lax.dot_general(a, b, (((1,), (1,)), ((), ())), preferred_element_type=F32)


def dot_tn(a, b):
    return lax.dot_general(a, b, (((0,), (0,)), ((), ())), preferred_element_type=F32)


def rotary_tables(length):
    positions = jnp.arange(length).astype(F32)
    exponents = jnp.arange(HALF).astype(F32) * (2.0 / HEAD_DIM)
    frequencies = jnp.exp(-math.log(500000.0) * exponents)
    angles = positions[:, None] * frequencies[None, :]
    cosine, sine = jnp.cos(angles), jnp.sin(angles)
    return (jnp.concatenate([cosine] * 4, 1), jnp.concatenate([sine] * 4, 1))


def first_half(shape):
    return lax.broadcasted_iota(jnp.int32, shape, 1) % HEAD_DIM < HALF


def ahead(value):
    return pltpu.roll(value, value.shape[1] - HALF, 1)


def behind(value):
    return pltpu.roll(value, HALF, 1)


def rotate(value, cosine, sine):
    turned = jnp.where(first_half(value.shape), -ahead(value), behind(value))
    return value * cosine + turned * sine


def rotate_back(grad, cosine, sine):
    scaled = grad * sine
    turned = jnp.where(first_half(grad.shape), ahead(scaled), -behind(scaled))
    return grad * cosine + turned


def block_start(core, x, offset):
    return pl.multiple_of((core * 4 + (x + offset) % 4) * BLOCK, BLOCK)


def attend_kernel(
    place, rows, gain, wq, wk, wv, wo, cosine, sine,
    mine_0, mine_1, mine_2, mine_3, other, own_input, normed, queries, keys, values, weights, context,
):
    core, x = place[0], place[1]
    length = rows.shape[0]
    gain_float = gain[...].astype(F32)
    for at in range(0, length, STRIP):
        strip = pl.ds(at, STRIP)
        rows_float = rows[strip, :].astype(F32)
        inv_rms = lax.rsqrt(jnp.mean(rows_float * rows_float, -1, keepdims=True) + 1e-05)
        normed[strip, :] = (rows_float * inv_rms * gain_float).astype(BF16)
    cos2, sin2 = cosine[...], sine[...]
    cos4, sin4 = jnp.concatenate([cos2, cos2], 1), jnp.concatenate([sin2, sin2], 1)
    all_normed = normed[...]
    queries[...] = rotate(dot(all_normed, wq[...]), cos4, sin4).astype(BF16)
    both = dot(all_normed, jnp.concatenate([wk[...], wv[...]], 1))
    keys[...] = rotate(both, cos2, sin2)[:, :HEAD_DIM].astype(BF16)
    values[...] = both[:, HEAD_DIM:].astype(BF16)
    heads = queries.shape[1] // HEAD_DIM
    for at in range(0, length, STRIP):
        strip, seen = pl.ds(at, STRIP), at + STRIP
        shape = (STRIP, seen)
        allowed = lax.broadcasted_iota(jnp.int32, shape, 1) <= at + lax.broadcasted_iota(
            jnp.int32, shape, 0
        )
        strip_queries = queries[strip, :]
        pieces = []
        for head in range(heads):
            query = strip_queries[:, head * HEAD_DIM : (head + 1) * HEAD_DIM]
            scores = dot_nt(query, keys[:seen, :]) * HEAD_DIM ** (-0.5)
            scores = jnp.where(allowed, scores, -1e30)
            exponent = jnp.exp(scores - jnp.max(scores, -1, keepdims=True))
            share = (exponent / jnp.sum(exponent, -1, keepdims=True)).astype(BF16)
            weights[head, strip, :seen] = share
            pieces.append(dot(share, values[:seen, :]))
        context[strip, :] = jnp.concatenate(pieces, 1).astype(BF16)
    own_input[...] = rows[:, pl.ds(block_start(core, x, 0), BLOCK)]
    all_context = context[...]
    for step, mine in enumerate((mine_0, mine_1, mine_2, mine_3)):
        there = wo[pl.ds(block_start(1 - core, x, step), BLOCK), :]
        other[step] = dot_nt(all_context, there).astype(BF16)
        here = wo[pl.ds(block_start(core, x, step), BLOCK), :]
        mine[...] = dot_nt(all_context, here).astype(BF16)


def pull_kernel(place, p0, p1, p2, p3, p4, p5, p6, p7, down, pulled, whole):
    core, x = place[0], place[1]
    for index, piece in enumerate((p0, p1, p2, p3, p4, p5, p6, p7)):
        side = core if index < 4 else 1 - core
        whole[:, pl.ds(block_start(side, x, 4 - index % 4), BLOCK)] = piece[...]
    pulled[...] = dot_nt(whole[...], down[...])


def server_kernel(
    place, p0, p1, p2, p3, p4, p5, p6, p7, pulled, gain, gate, up,
    mine_0, mine_1, mine_2, mine_3, other, normed, grads,
):
    core, x = place[0], place[1]
    pieces = (p0, p1, p2, p3, p4, p5, p6, p7)
    width = gate.shape[0]
    starts = [
        block_start(core if index < 4 else 1 - core, x, 4 - index % 4) for index in range(8)
    ]
    squares = jnp.zeros((p0.shape[0], 1), F32)
    for piece in pieces:
        rows_float = piece[...].astype(F32)
        squares = squares + jnp.sum(rows_float * rows_float, -1, keepdims=True)
    inv_rms = lax.rsqrt(squares / width + 1e-05)
    for piece, start in zip(pieces, starts):
        gain_float = gain[:, pl.ds(start, BLOCK)].astype(F32)
        normed[:, pl.ds(start, BLOCK)] = (piece[...].astype(F32) * inv_rms * gain_float).astype(BF16)
    gate_value = dot(normed[...], gate[...])
    up_value = dot(normed[...], up[...])
    sigmoid_gate = jax.nn.sigmoid(gate_value)
    pull = pulled[...]
    gate_grad = (
        pull * up_value * sigmoid_gate * (1.0 + gate_value * (1.0 - sigmoid_gate))
    ).astype(BF16)
    up_grad = (pull * gate_value * sigmoid_gate).astype(BF16)
    along = jnp.zeros((p0.shape[0], 1), F32)
    for index, (piece, start) in enumerate(zip(pieces, starts)):
        some = pl.ds(start, BLOCK)
        weighted = dot_nt(gate_grad, gate[some, :]) + dot_nt(up_grad, up[some, :])
        weighted = weighted * gain[:, some].astype(F32)
        grads[index] = weighted
        along = along + jnp.sum(weighted * piece[...].astype(F32), -1, keepdims=True)
    scale = inv_rms * inv_rms * inv_rms * (along / width)
    mine = (mine_0, mine_1, mine_2, mine_3)
    for index, piece in enumerate(pieces):
        part = (inv_rms * grads[index] - piece[...].astype(F32) * scale).astype(BF16)
        step = (4 - index % 4) % 4
        if index < 4:
            mine[step][...] = part
        else:
            other[step] = part


def output_kernel(
    place, p0, p1, p2, p3, p4, p5, p6, p7, wo, context, context_grad, t0, t1, t2, t3, arrived, tall
):
    core, x, y = place[0], place[1], place[2]
    all_context = context[...]
    for index, piece in enumerate((p0, p1, p2, p3, p4, p5, p6, p7)):
        side = core if index < 4 else 1 - core
        some = pl.ds(block_start(side, x, 4 - index % 4), BLOCK)
        rows = piece[...]
        arrived[:, some] = rows
        tall[some, :] = dot_tn(rows, all_context).astype(BF16)
    context_grad[...] = dot(arrived[...], wo[...]).astype(BF16)
    for step, target in enumerate((t0, t1, t2, t3)):
        there = (y + step) % 4
        for z in range(8):
            row = (((there % 2) * 8 + z) * 2 + there // 2) * 64
            target[z] = tall[pl.ds(pl.multiple_of(row, 64), 64), :]


def attend_back_kernel(
    place, context_grad, turned, queries, keys, values, weights, cosine, sine,
    t0, t1, t2, t3, t4, t5, t6, t7, joined, tall,
):
    y, z = place[2], place[3]
    length = queries.shape[0]
    heads = queries.shape[1] // HEAD_DIM
    key_grad = [jnp.zeros((STRIP, HEAD_DIM), F32)] * (length // STRIP)
    value_grad = [jnp.zeros((STRIP, HEAD_DIM), F32)] * (length // STRIP)
    cos2, sin2 = cosine[...], sine[...]
    cos4, sin4 = jnp.concatenate([cos2, cos2], 1), jnp.concatenate([sin2, sin2], 1)
    for at in range(0, length, STRIP):
        strip, seen = pl.ds(at, STRIP), at + STRIP
        strip_queries, strip_grads = queries[strip, :], context_grad[strip, :]
        pieces = []
        for head in range(heads):
            part = slice(head * HEAD_DIM, (head + 1) * HEAD_DIM)
            share = weights[head, strip, :seen]
            share_float = share.astype(F32)
            ahead_grad = dot_nt(strip_grads[:, part], values[:seen, :]).astype(BF16).astype(F32)
            level = jnp.sum(ahead_grad * share_float, -1, keepdims=True)
            score_grad = (share_float * (ahead_grad - level) * HEAD_DIM ** (-0.5)).astype(BF16)
            pieces.append(dot(score_grad, keys[:seen, :]))
            for_keys = dot_tn(score_grad, strip_queries[:, part])
            for_values = dot_tn(share, strip_grads[:, part])
            for block in range(seen // STRIP):
                rows = slice(block * STRIP, (block + 1) * STRIP)
                key_grad[block] = key_grad[block] + for_keys[rows]
                value_grad[block] = value_grad[block] + for_values[rows]
        query_grad = jnp.concatenate(pieces, 1).astype(BF16).astype(F32)
        joined[strip, :BLOCK] = rotate_back(
            query_grad, cos4[at:seen], sin4[at:seen]
        ).astype(BF16)
    for block in range(length // STRIP):
        rows = slice(block * STRIP, (block + 1) * STRIP)
        of_keys = key_grad[block].astype(BF16).astype(F32)
        pair = jnp.concatenate([of_keys, value_grad[block].astype(BF16).astype(F32)], 1)
        back = rotate_back(pair, cos2[rows], sin2[rows])
        lane = lax.broadcasted_iota(jnp.int32, pair.shape, 1)
        joined[pl.ds(block * STRIP, STRIP), BLOCK:] = jnp.where(
            lane < HEAD_DIM, back, pair
        ).astype(BF16)
    tall[...] = dot(turned[...], joined[...]).astype(BF16)
    for step, target in enumerate((t0, t1, t2, t3, t4, t5, t6, t7)):
        at_z = (z + step) % 8
        for move in range(4):
            there = (y + move) % 4
            row = (((there % 2) * 8 + at_z) * 2 + there // 2) * 64
            target[move] = tall[pl.ds(pl.multiple_of(row, 64), 64), :]


def x_shift(value, step):
    size = lax.axis_size("x")
    return lax.ppermute(value, "x", [(i, (i + step) % size) for i in range(size)])


def core_swap(value):
    return lax.ppermute(value, "core", [(0, 1), (1, 0)])


def group_swap(value):
    return lax.ppermute(value, "yh", [(0, 1), (1, 0)])


def y_shift(value, step):
    def place(y):
        return (y % 2) * 2 + y // 2

    return lax.ppermute(value, ("yl", "yh"), [(place(y), place((y + step) % 4)) for y in range(4)])


def z_shift(value, step):
    size = lax.axis_size("z")
    return lax.ppermute(value, "z", [(i, (i + step) % size) for i in range(size)])


def over_clients(pieces):
    return lax.all_to_all(pieces, ("yl", "z"), 0, 0, tiled=True)


def pick(pieces, order):
    return pieces.at[order].get(mode="promise_in_bounds")


def added(*terms):
    return sum(term.astype(F32) for term in terms)


def relay_out(rows, keep, send):
    pieces = over_clients(rows.reshape(16, -1, BLOCK))
    arrived = group_swap(pick(pieces, send))
    return jnp.concatenate([pick(pieces, keep), arrived], 0).reshape(rows.shape)


def relay_back(rows, inverse):
    pieces = rows.reshape(16, -1, BLOCK)
    returned = group_swap(pieces[8:])
    ordered = pick(jnp.concatenate([pieces[:8], returned], 0), inverse)
    return over_clients(ordered).reshape(rows.shape)


def share_sum(mine, other, *more):
    arrived = core_swap(other)
    pairs = [added(mine[step], arrived[step]) for step in range(4)]
    parts = [x_shift(pairs[step].astype(BF16), step) for step in (1, 3, 2)]
    return added(pairs[0], *parts, *more).astype(BF16)


def widen_rows(own):
    mine = [own] + [x_shift(own, step) for step in (1, 2, 3)]
    return mine + [core_swap(piece) for piece in mine]


def local(
    client_input,
    client_gain,
    query_weight,
    key_weight,
    client_value_weight,
    output_weight,
    server_gain,
    server_gate,
    server_up,
    server_down,
    upstream,
    assignment,
):
    length = client_input.shape[0]
    x, core, group = lax.axis_index("x"), lax.axis_index("core"), lax.axis_index("yh")
    place = jnp.stack([core, x, group * 2 + lax.axis_index("yl"), lax.axis_index("z")])
    leaves = (assignment != group).astype(jnp.int32)
    clients = jnp.arange(16)
    before = (clients[:, None] > clients[None, :]) & (leaves[:, None] == leaves[None, :])
    inverse = jnp.sum(before.astype(jnp.int32), 1) + 8 * leaves
    order = jnp.sum(jnp.where(inverse[None, :] == clients[:, None], clients[None, :], 0), 1)
    keep, send = order[:8], order[8:]
    cosine, sine = rotary_tables(length)

    own_upstream = lax.dynamic_slice_in_dim(upstream, (core * 4 + x) * BLOCK, BLOCK, 1)
    server_upstream = relay_out(own_upstream, keep, send)
    wide_upstream = widen_rows(server_upstream)
    (pulled,) = on_core(
        pull_kernel,
        [((length, server_down.shape[1]), F32)],
        [pltpu.VMEM(client_input.shape, BF16)],
    )(place, *wide_upstream, server_down[0])

    piece, stack = ((length, BLOCK), BF16), ((4, length, BLOCK), BF16)
    head = ((length, HEAD_DIM), BF16)
    heads = query_weight.shape[2] // HEAD_DIM
    fwd = on_core(
        attend_kernel,
        [piece] * 4
        + [stack, piece, (client_input.shape, BF16), piece, head, head]
        + [((heads, length, length), BF16), piece],
    )(
        place, client_input, client_gain, query_weight[0], key_weight[0],
        client_value_weight[0], output_weight[0], cosine, sine,
    )
    mine, other, (own_input, normed, queries, keys, values, weights, context) = (
        fwd[:4], fwd[4], fwd[5:],
    )
    cut_input = share_sum(mine, other, own_input)
    wide_rows = widen_rows(relay_out(cut_input, keep, send))
    back = on_core(
        server_kernel,
        [piece] * 4 + [stack],
        [pltpu.VMEM(client_input.shape, BF16), pltpu.VMEM((8, length, BLOCK), F32)],
    )(place, *wide_rows, pulled, server_gain, server_gate[0], server_up[0])
    cut_grad = share_sum(back[:4], back[4], server_upstream)
    arriving = widen_rows(relay_back(cut_grad, inverse))
    width = client_input.shape[1]
    context_grad, *outs = on_core(
        output_kernel,
        [piece] + [((8, 64, BLOCK), BF16)] * 4,
        [pltpu.VMEM(client_input.shape, BF16), pltpu.VMEM((width, BLOCK), BF16)],
    )(place, *arriving, output_weight[0], context)
    joined_width = BLOCK + 2 * HEAD_DIM
    tiles = on_core(
        attend_back_kernel,
        [((4, 64, joined_width), BF16)] * 8,
        [pltpu.VMEM((length, joined_width), BF16), pltpu.VMEM((width, joined_width), BF16)],
    )(place, context_grad, normed.T, queries, keys, values, weights, cosine, sine)

    out_sum = added(outs[0], *[y_shift(outs[step], step) for step in (1, 3, 2)]).astype(BF16)
    out_total = added(*lax.all_to_all(out_sum, "z", 0, 0, tiled=True))
    output_update = (out_total / 16).astype(BF16)

    up = z_shift(tiles[4][:2], 1)
    down = z_shift(tiles[4][2:], -1)
    rising = jnp.concatenate([added(tiles[3][:2], up).astype(BF16), tiles[3][2:]], 0)
    falling = jnp.concatenate([tiles[5][:2], added(tiles[5][2:], down).astype(BF16)], 0)
    for step in (2, 1, 0):
        up, down = z_shift(rising, 1), z_shift(falling, -1)
        if step:
            rising = added(tiles[step], up).astype(BF16)
            falling = added(tiles[8 - step], down).astype(BF16)
    held = added(tiles[0], up, down)
    rounded = held.astype(BF16)
    total = added(held[0], *[y_shift(rounded[step], step) for step in (1, 3, 2)])
    total = (total / 16).astype(BF16)
    return (
        total[:, :BLOCK],
        total[:, BLOCK : BLOCK + HEAD_DIM],
        total[:, BLOCK + HEAD_DIM :],
        output_update,
    )


def solution(mesh):
    fine = Mesh(mesh.devices.reshape(2, 8, 4, 2, 2), ("yl", "z", "x", "core", "yh"))
    client, tensor, sdata = ("yl", "z"), ("x", "core"), "yh"
    rows = ("yl", "z", "yh")
    placed = (
        P(rows, None),
        P(client, None),
        P(client, None, tensor),
        P(client, None, tensor),
        P(client, None, tensor),
        P(client, None, tensor),
        P(sdata, None),
        P(sdata, None, tensor),
        P(sdata, None, tensor),
        P(sdata, tensor, None),
        P(rows, None),
        P(),
    )
    return jax.shard_map(
        local,
        mesh=fine,
        in_specs=placed,
        out_specs=(P(rows, tensor), P(rows, tensor), P(rows, tensor), P(rows, tensor)),
        check_vma=False,
    )
```

```python
import jax
import jax.numpy as jnp
import numpy as np
from jax import lax
from jax.experimental import pallas as pl
from jax.experimental.pallas import tpu as pltpu
from jax.sharding import Mesh, PartitionSpec as P

HEAD_DIM = 64
HALF = HEAD_DIM // 2
BLOCK = 256
STRIP = 128
F32 = jnp.float32
BF16 = jnp.bfloat16
SMEM = pl.BlockSpec(memory_space=pltpu.SMEM)
VMEM = pl.BlockSpec(memory_space=pltpu.VMEM)


def on_core(kernel, outputs, scratch=()):
    def call(place, *operands):
        return pl.pallas_call(
            kernel,
            out_shape=[jax.ShapeDtypeStruct(shape, kind) for shape, kind in outputs],
            in_specs=[SMEM] + [VMEM] * len(operands),
            out_specs=[VMEM] * len(outputs),
            scratch_shapes=list(scratch),
            compiler_params=pltpu.CompilerParams(vmem_limit_bytes=60 * 1024 * 1024),
        )(place, *operands)

    return call


def dot(a, b):
    return jnp.dot(a, b, preferred_element_type=F32)


def dot_nt(a, b):
    return lax.dot_general(a, b, (((1,), (1,)), ((), ())), preferred_element_type=F32)


def dot_tn(a, b):
    return lax.dot_general(a, b, (((0,), (0,)), ((), ())), preferred_element_type=F32)


def rotary_tables(length):
    angles = np.arange(max(length // 16, 16))[:, None] * 500000.0 ** (-np.arange(HALF) * 2 / HEAD_DIM)
    wide = np.concatenate([angles] * 4, 1)
    fine, coarse = wide[:16], 16 * wide[: length // 16]
    return [np.float32(f(t)) for t in (fine, coarse) for f in (np.cos, np.sin)]


def expand_tables(fine_cos, fine_sin, coarse_cos, coarse_sin):
    near_cos, near_sin = fine_cos[...][None], fine_sin[...][None]
    far_cos, far_sin = coarse_cos[...][:, None], coarse_sin[...][:, None]
    shape = (far_cos.shape[0] * 16, far_cos.shape[2])
    cosine = (far_cos * near_cos - far_sin * near_sin).reshape(shape)
    sine = (far_sin * near_cos + far_cos * near_sin).reshape(shape)
    return cosine, sine


def first_half(shape):
    return lax.broadcasted_iota(jnp.int32, shape, 1) % HEAD_DIM < HALF


def ahead(value):
    return pltpu.roll(value, value.shape[1] - HALF, 1)


def behind(value):
    return pltpu.roll(value, HALF, 1)


def rotate(value, cosine, sine):
    turned = jnp.where(first_half(value.shape), -ahead(value), behind(value))
    return value * cosine + turned * sine


def rotate_back(grad, cosine, sine):
    scaled = grad * sine
    turned = jnp.where(first_half(grad.shape), ahead(scaled), -behind(scaled))
    return grad * cosine + turned


def block_start(core, x, offset):
    return pl.multiple_of((core * 4 + (x + offset) % 4) * BLOCK, BLOCK)


def attend_kernel(
    place, rows, gain, wq, wk, wv, wo, fine_cos, fine_sin, coarse_cos, coarse_sin,
    mine, other, own_input, normed, queries, keys, values, weights, context,
    parts,
):
    core, x = place[0], place[1]
    length, heads = rows.shape[0], queries.shape[0]
    gain_float = gain[...].astype(F32)

    @pl.loop(0, length // STRIP)
    def _(at):
        strip = pl.ds(pl.multiple_of(at * STRIP, STRIP), STRIP)
        rows_float = rows[strip, :].astype(F32)
        inv_rms = lax.rsqrt(jnp.mean(rows_float * rows_float, -1, keepdims=True) + 1e-05)
        normed[strip, :] = (rows_float * inv_rms * gain_float).astype(BF16)

    cos2, sin2 = expand_tables(fine_cos, fine_sin, coarse_cos, coarse_sin)
    cos4, sin4 = jnp.concatenate([cos2, cos2], 1), jnp.concatenate([sin2, sin2], 1)
    all_normed = normed[...]
    all_queries = rotate(dot(all_normed, wq[...]), cos4, sin4).astype(BF16)
    for head in range(heads):
        queries[head] = all_queries[:, head * HEAD_DIM : (head + 1) * HEAD_DIM]
    both = dot_nt(all_normed, jnp.concatenate([wk[...], wv[...]], 0))
    keys[...] = rotate(both, cos2, sin2)[:, :HEAD_DIM].astype(BF16)
    values[...] = both[:, HEAD_DIM:].astype(BF16)
    for at in range(0, length, STRIP):
        strip, seen = pl.ds(at, STRIP), at + STRIP
        shape = (STRIP, seen)
        allowed = lax.broadcasted_iota(jnp.int32, shape, 1) <= at + lax.broadcasted_iota(
            jnp.int32, shape, 0
        )

        @pl.loop(0, heads, unroll=4)
        def _(head):
            scores = dot_nt(queries[head, strip, :], keys[:seen, :]) * HEAD_DIM ** (-0.5)
            scores = jnp.where(allowed, scores, -1e30)
            exponent = jnp.exp(scores - jnp.max(scores, -1, keepdims=True))
            share = (exponent / jnp.sum(exponent, -1, keepdims=True)).astype(BF16)
            weights[head, strip, :seen] = share
            parts[head, strip, :] = dot(share, values[:seen, :])

    context[...] = jnp.concatenate([parts[head] for head in range(heads)], 1).astype(BF16)
    own_input[...] = rows[:, pl.ds(block_start(core, x, 0), BLOCK)]

    @pl.loop(0, 4)
    def _(step):
        there = wo[pl.ds(block_start(1 - core, x, step), BLOCK), :]
        other[step] = dot_nt(context[...], there).astype(BF16)
        here = wo[pl.ds(block_start(core, x, step), BLOCK), :]
        mine[step] = dot_nt(context[...], here).astype(BF16)


def spread(tall, y, targets):
    for step, target in enumerate(targets):
        there = (y + step) % 4

        @pl.loop(0, 8)
        def _(z):
            row = (((there % 2) * 8 + z) * 2 + there // 2) * 64
            target[z] = tall[pl.ds(pl.multiple_of(row, 64), 64), :]


def pull_kernel(place, kept, moved, kept_there, moved_there, down, pulled, own_upstream, whole):
    core, x = place[0], place[1]
    rows, wide = kept.shape
    sides = ((core, (kept, moved)), (1 - core, (kept_there, moved_there)))
    for side, halves in sides:
        for half, piece in enumerate(halves):
            start = pl.multiple_of(side * wide, wide)
            whole[pl.ds(half * rows, rows), pl.ds(start, wide)] = piece[...]
    own_upstream[...] = whole[:, pl.ds(block_start(core, x, 0), BLOCK)]
    pulled[...] = dot_nt(whole[...], down[...])


def server_kernel(
    place, p0, p1, p2, p3, q0, q1, pulled, gain, gate, up,
    mine, other, normed, grads, gates, ups, gate_grad, up_grad, inverse,
):
    core, x = place[0], place[1]
    pieces = (p0, p1, p2, p3, q0, q1.at[0], q1.at[1], q1.at[2])
    width, length = gate.shape[0], p0.shape[0]
    blocks = [
        pl.ds(block_start(core if index < 4 else 1 - core, x, 4 - index % 4), BLOCK)
        for index in range(8)
    ]

    def strips(step):
        @pl.loop(0, length // STRIP)
        def _(at):
            step(pl.ds(pl.multiple_of(at * STRIP, STRIP), STRIP))

    def normalize(strip):
        squares = jnp.zeros((STRIP, 1), F32)
        for piece in pieces:
            rows_float = piece[strip, :].astype(F32)
            squares = squares + jnp.sum(rows_float * rows_float, -1, keepdims=True)
        inv_rms = lax.rsqrt(squares / width + 1e-05)
        inverse[strip, :] = inv_rms
        for piece, some in zip(pieces, blocks):
            scaled = piece[strip, :].astype(F32) * inv_rms * gain[:, some].astype(F32)
            normed[strip, some] = scaled.astype(BF16)

    strips(normalize)
    gates[...] = dot(normed[...], gate[...])
    ups[...] = dot(normed[...], up[...])

    def through_gate(strip):
        gate_value, pull = gates[strip, :], pulled[strip, :]
        sigmoid_gate = jax.nn.sigmoid(gate_value)
        slope = sigmoid_gate * (1.0 + gate_value * (1.0 - sigmoid_gate))
        gate_grad[strip, :] = (pull * ups[strip, :] * slope).astype(BF16)
        up_grad[strip, :] = (pull * gate_value * sigmoid_gate).astype(BF16)

    strips(through_gate)
    for index, some in enumerate(blocks):
        grads[index] = dot_nt(gate_grad[...], gate[some, :]) + dot_nt(up_grad[...], up[some, :])

    def finish(strip):
        along = jnp.zeros((STRIP, 1), F32)
        for index, (piece, some) in enumerate(zip(pieces, blocks)):
            weighted = grads[index, strip, :] * gain[:, some].astype(F32)
            grads[index, strip, :] = weighted
            along = along + jnp.sum(weighted * piece[strip, :].astype(F32), -1, keepdims=True)
        inv_rms = inverse[strip, :]
        scale = inv_rms * inv_rms * inv_rms * (along / width)
        for index, piece in enumerate(pieces):
            part = inv_rms * grads[index, strip, :] - piece[strip, :].astype(F32) * scale
            step = (4 - index % 4) % 4
            if index < 4:
                mine[step, strip, :] = part.astype(BF16)
            else:
                other[step, strip, :] = part.astype(BF16)

    strips(finish)


def output_kernel(
    place, p0, p1, p2, p3, q0, q1, wo, context, context_grad, t0, t1, t2, t3, arrived, tall
):
    core, x = place[0], place[1]
    pieces = (p0, p1, p2, p3, q0, q1.at[0], q1.at[1], q1.at[2])
    for index, piece in enumerate(pieces):
        side = core if index < 4 else 1 - core
        some = pl.ds(block_start(side, x, 4 - index % 4), BLOCK)
        rows = piece[...]
        arrived[:, some] = rows
        tall[some, :] = dot_tn(rows, context[...]).astype(BF16)
    grads = dot(arrived[...], wo[...]).astype(BF16)
    for head in range(context_grad.shape[0]):
        context_grad[head] = grads[:, head * HEAD_DIM : (head + 1) * HEAD_DIM]
    spread(tall, place[2], (t0, t1, t2, t3))


def attend_back_kernel(
    place, context_grad, turned, queries, keys, values, weights, fine_cos, fine_sin, coarse_cos, coarse_sin,
    t0, t1, t2, t3, joined, tall, query_grad, key_grad, value_grad,
):
    heads, length = queries.shape[0], queries.shape[1]
    cos2, sin2 = expand_tables(fine_cos, fine_sin, coarse_cos, coarse_sin)
    cos4, sin4 = jnp.concatenate([cos2, cos2], 1), jnp.concatenate([sin2, sin2], 1)
    key_grad[...] = jnp.zeros_like(key_grad)
    value_grad[...] = jnp.zeros_like(value_grad)
    for at in range(0, length, STRIP):
        strip, seen = pl.ds(at, STRIP), at + STRIP

        @pl.loop(0, heads, unroll=2)
        def _(head):
            share, grads = weights[head, strip, :seen], context_grad[head, strip, :]
            share_float = share.astype(F32)
            share_grad = dot_nt(grads, values[:seen, :]).astype(BF16).astype(F32)
            level = jnp.sum(share_grad * share_float, -1, keepdims=True)
            score_grad = (share_float * (share_grad - level) * HEAD_DIM ** (-0.5)).astype(BF16)
            query_grad[head, strip, :] = dot(score_grad, keys[:seen, :])
            key_grad[:seen, :] += dot_tn(score_grad, queries[head, strip, :])
            value_grad[:seen, :] += dot_tn(share, grads)

    of_queries = jnp.concatenate([query_grad[head] for head in range(heads)], 1)
    joined[:, :BLOCK] = rotate_back(of_queries.astype(BF16).astype(F32), cos4, sin4).astype(BF16)
    pair = jnp.concatenate([key_grad[...], value_grad[...]], 1).astype(BF16).astype(F32)
    lane = lax.broadcasted_iota(jnp.int32, pair.shape, 1)
    back = jnp.where(lane < HEAD_DIM, rotate_back(pair, cos2, sin2), pair)
    joined[:, BLOCK:] = back.astype(BF16)
    tall[...] = dot(turned[...], joined[...]).astype(BF16)
    spread(tall, place[2], (t0, t1, t2, t3))


def x_shift(value, step):
    size = lax.axis_size("x")
    return lax.ppermute(value, "x", [(i, (i + step) % size) for i in range(size)])


def core_swap(value):
    return lax.ppermute(value, "core", [(0, 1), (1, 0)])


def group_swap(value):
    return lax.ppermute(value, "yh", [(0, 1), (1, 0)])


def y_shift(value, step):
    def place(y):
        return (y % 2) * 2 + y // 2

    return lax.ppermute(value, ("yl", "yh"), [(place(y), place((y + step) % 4)) for y in range(4)])


def over_clients(pieces):
    return lax.all_to_all(pieces, ("yl", "z"), 0, 0, tiled=True)


def pick(pieces, order):
    return pieces.at[order].get(mode="promise_in_bounds")


def added(*terms):
    return sum(term.astype(F32) for term in terms)


def relay_out(rows, order):
    pieces = over_clients(rows.reshape(16, -1, rows.shape[1]))
    arrived = group_swap(pick(pieces, order[8:]))
    return pieces, arrived


def relay_back(rows, inverse):
    pieces = rows.reshape(16, -1, BLOCK)
    returned = group_swap(pieces[8:])
    ordered = pick(jnp.concatenate([pieces[:8], returned], 0), inverse)
    return over_clients(ordered).reshape(rows.shape)


def share_sum(mine, other, *more):
    arrived = core_swap(other)
    pairs = [added(mine[step], arrived[step]) for step in range(4)]
    parts = [x_shift(pairs[step].astype(BF16), step) for step in (1, 3, 2)]
    return added(pairs[0], *parts, *more).astype(BF16)


def widen_rows(own):
    parts = [x_shift(own, step) for step in (1, 3, 2)]
    rest = [parts[0], parts[2], parts[1]]
    return [own, *rest, core_swap(own), core_swap(jnp.stack(rest))]


def tile_sum(tiles):
    parts = [y_shift(tiles[step], step) for step in (1, 3, 2)]
    summed = added(tiles[0], *parts).astype(BF16)
    pieces = lax.all_to_all(summed, "z", 0, 0, tiled=True)
    return (added(*pieces) / 16).astype(BF16)


def local(
    client_input,
    client_gain,
    query_weight,
    key_weight,
    client_value_weight,
    output_weight,
    server_gain,
    server_gate,
    server_up,
    server_down,
    upstream,
    assignment,
):
    length = client_input.shape[0]
    x, core, group = lax.axis_index("x"), lax.axis_index("core"), lax.axis_index("yh")
    at, y = jnp.arange(3), group * 2 + lax.axis_index("yl")
    place = jnp.where(at == 0, core, jnp.where(at == 1, x, y))
    leaves = (assignment != group).astype(jnp.int32)
    clients = jnp.arange(16)
    before = (clients[:, None] > clients[None, :]) & (leaves[:, None] == leaves[None, :])
    inverse = jnp.sum(before.astype(jnp.int32), 1) + 8 * leaves
    order = jnp.sum(jnp.where(inverse[None, :] == clients[:, None], clients[None, :], 0), 1)
    tables = rotary_tables(length)

    half = 4 * BLOCK
    own_upstream = lax.dynamic_slice_in_dim(upstream, core * half, half, 1)
    piece, stack = ((length, BLOCK), BF16), ((4, length, BLOCK), BF16)
    head = ((length, HEAD_DIM), BF16)
    heads = query_weight.shape[2] // HEAD_DIM
    by_head = ((heads, length, HEAD_DIM), BF16)
    fwd = on_core(
        attend_kernel,
        [stack, stack, piece, (client_input.shape, BF16), by_head, head, head]
        + [((heads, length, length), BF16), piece],
        [pltpu.VMEM((heads, length, HEAD_DIM), F32)],
    )(
        place, client_input, client_gain, query_weight[0], key_weight[0].T,
        client_value_weight[0].T, output_weight[0], *tables,
    )
    mine, other, (own_input, normed, queries, keys, values, weights, context) = (
        fwd[0], fwd[1], fwd[2:],
    )
    pieces, moved = relay_out(own_upstream, order)
    kept = pick(pieces, order[:8]).reshape(-1, half)
    moved = moved.reshape(-1, half)
    there = (core_swap(kept), core_swap(moved))
    pulled, server_upstream = on_core(
        pull_kernel,
        [((length, server_down.shape[1]), F32), piece],
        [pltpu.VMEM(client_input.shape, BF16)],
    )(place, kept, moved, *there, server_down[0])
    turned = normed.T
    pulled, turned = lax.optimization_barrier((pulled, turned))
    cut_input = share_sum(mine, other, own_input)
    pieces, moved = relay_out(cut_input, order)
    arranged = lax.dynamic_update_slice_in_dim(pick(pieces, order), moved, 8, 0)
    wide_rows = widen_rows(arranged.reshape(length, BLOCK))
    back = on_core(
        server_kernel,
        [stack, stack],
        [
            pltpu.VMEM(client_input.shape, BF16),
            pltpu.VMEM((8, length, BLOCK), F32),
            pltpu.VMEM((length, server_gate.shape[2]), F32),
            pltpu.VMEM((length, server_gate.shape[2]), F32),
            pltpu.VMEM((length, server_gate.shape[2]), BF16),
            pltpu.VMEM((length, server_gate.shape[2]), BF16),
            pltpu.VMEM((length, 1), F32),
        ],
    )(place, *wide_rows, pulled, server_gain, server_gate[0], server_up[0])
    cut_grad = share_sum(back[0], back[1], server_upstream)
    arriving = widen_rows(relay_back(cut_grad, inverse))
    width = client_input.shape[1]
    context_grad, *outs = on_core(
        output_kernel,
        [by_head] + [((8, 64, BLOCK), BF16)] * 4,
        [pltpu.VMEM(client_input.shape, BF16), pltpu.VMEM((width, BLOCK), BF16)],
    )(place, *arriving, output_weight[0], context)
    joined_width = BLOCK + 2 * HEAD_DIM
    tiles = on_core(
        attend_back_kernel,
        [((8, 64, joined_width), BF16)] * 4,
        [
            pltpu.VMEM((length, joined_width), BF16),
            pltpu.VMEM((width, joined_width), BF16),
            pltpu.VMEM((heads, length, HEAD_DIM), F32),
            pltpu.VMEM((length, HEAD_DIM), F32),
            pltpu.VMEM((length, HEAD_DIM), F32),
        ],
    )(place, context_grad, turned, queries, keys, values, weights, *tables)
    output_update = tile_sum(outs)
    total = tile_sum(tiles)
    return (
        total[:, :BLOCK],
        total[:, BLOCK : BLOCK + HEAD_DIM],
        total[:, BLOCK + HEAD_DIM :],
        output_update,
    )


def solution(mesh):
    fine = Mesh(mesh.devices.reshape(2, 8, 4, 2, 2), ("yl", "z", "x", "core", "yh"))
    client, tensor, sdata = ("yl", "z"), ("x", "core"), "yh"
    rows = ("yl", "z", "yh")
    placed = (
        P(rows, None),
        P(client, None),
        P(client, None, tensor),
        P(client, None, tensor),
        P(client, None, tensor),
        P(client, None, tensor),
        P(sdata, None),
        P(sdata, None, tensor),
        P(sdata, None, tensor),
        P(sdata, tensor, None),
        P(rows, None),
        P(),
    )
    return jax.shard_map(
        local,
        mesh=fine,
        in_specs=placed,
        out_specs=(P(rows, tensor), P(rows, tensor), P(rows, tensor), P(rows, tensor)),
        check_vma=False,
    )
```

```python
import jax
import jax.numpy as jnp
import numpy as np
from jax import lax
from jax.experimental import pallas as pl
from jax.experimental.pallas import tpu as pltpu
from jax.sharding import Mesh, PartitionSpec as P

HEAD_DIM = 64
HALF = HEAD_DIM // 2
BLOCK = 256
STRIP = 128
F32 = jnp.float32
BF16 = jnp.bfloat16
SMEM = pl.BlockSpec(memory_space=pltpu.SMEM)
VMEM = pl.BlockSpec(memory_space=pltpu.VMEM)


ANY = pl.BlockSpec(memory_space=pl.ANY)


class Late:
    def __init__(self, source, target, semaphore):
        self.copy, self.target = pltpu.make_async_copy(source, target, semaphore), target
        self.copy.start()

    def ready(self):
        self.copy.wait()
        return self.target


def on_core(kernel, outputs, scratch=(), late=(), limit=24):
    def call(place, *operands):
        count = len(operands)
        kept = count + len(outputs) + len(scratch)

        def body(place, *refs):
            semaphores = refs[-1]
            values = list(refs[:count])
            for at, index in enumerate(late):
                values[index] = Late(refs[index], refs[kept + at], semaphores.at[at])
            kernel(place, *values, *refs[count:kept])

        buffers = [pltpu.VMEM(operands[index].shape, operands[index].dtype) for index in late]
        return pl.pallas_call(
            body,
            out_shape=[jax.ShapeDtypeStruct(shape, kind) for shape, kind in outputs],
            in_specs=[SMEM] + [ANY if index in late else VMEM for index in range(count)],
            out_specs=[VMEM] * len(outputs),
            scratch_shapes=[
                *scratch,
                *buffers,
                pltpu.SemaphoreType.DMA((max(len(late), 1),)),
            ],
            compiler_params=pltpu.CompilerParams(vmem_limit_bytes=limit * 1024 * 1024),
        )(place, *operands)

    return call


def dot(a, b):
    return jnp.dot(a, b, preferred_element_type=F32)


def dot_nt(a, b):
    return lax.dot_general(a, b, (((1,), (1,)), ((), ())), preferred_element_type=F32)


def dot_tn(a, b):
    return lax.dot_general(a, b, (((0,), (0,)), ((), ())), preferred_element_type=F32)


def rotary_tables(length):
    angles = np.arange(max(length // 16, 16))[:, None] * 500000.0 ** (-np.arange(HALF) * 2 / HEAD_DIM)
    wide = np.concatenate([angles] * 4, 1)
    fine, coarse = wide[:16], 16 * wide[: length // 16]
    return [np.float32(f(t)) for t in (fine, coarse) for f in (np.cos, np.sin)]


def expand_tables(fine_cos, fine_sin, coarse_cos, coarse_sin):
    near_cos, near_sin = fine_cos[...][None], fine_sin[...][None]
    far_cos, far_sin = coarse_cos[...][:, None], coarse_sin[...][:, None]
    shape = (far_cos.shape[0] * 16, far_cos.shape[2])
    cosine = (far_cos * near_cos - far_sin * near_sin).reshape(shape)
    sine = (far_sin * near_cos + far_cos * near_sin).reshape(shape)
    return cosine, sine


def first_half(shape):
    return lax.broadcasted_iota(jnp.int32, shape, 1) % HEAD_DIM < HALF


def ahead(value):
    return pltpu.roll(value, value.shape[1] - HALF, 1)


def behind(value):
    return pltpu.roll(value, HALF, 1)


def rotate(value, cosine, sine):
    turned = jnp.where(first_half(value.shape), -ahead(value), behind(value))
    return value * cosine + turned * sine


def rotate_back(grad, cosine, sine):
    scaled = grad * sine
    turned = jnp.where(first_half(grad.shape), ahead(scaled), -behind(scaled))
    return grad * cosine + turned


def normalize(rows, gain, strip):
    rows_float = rows[strip, :].astype(F32)
    inv_rms = lax.rsqrt(jnp.mean(rows_float * rows_float, -1, keepdims=True) + 1e-05)
    return (rows_float * inv_rms * gain[...].astype(F32)).astype(BF16)


def block_start(core, x, offset):
    return pl.multiple_of((core * 4 + (x + offset) % 4) * BLOCK, BLOCK)


def attend_kernel(
    place, rows, gain, wq, wk, wv, wo, fine_cos, fine_sin, coarse_cos, coarse_sin,
    mine, other, own_input, queries, keys, values, weights, context,
    parts, normed,
):
    core, x = place[0], place[1]
    length, heads = normed.shape[0], queries.shape[0]

    @pl.loop(0, length // STRIP)
    def _(at):
        strip = pl.ds(pl.multiple_of(at * STRIP, STRIP), STRIP)
        normed[strip, :] = normalize(rows, gain, strip)

    cos2, sin2 = expand_tables(fine_cos, fine_sin, coarse_cos, coarse_sin)
    cos4, sin4 = jnp.concatenate([cos2, cos2], 1), jnp.concatenate([sin2, sin2], 1)
    all_normed = normed[...]
    all_queries = rotate(dot(all_normed, wq[...]), cos4, sin4).astype(BF16)
    for head in range(heads):
        queries[head] = all_queries[:, head * HEAD_DIM : (head + 1) * HEAD_DIM]
    both = dot_nt(all_normed, jnp.concatenate([wk[...], wv[...]], 0))
    keys[...] = rotate(both, cos2, sin2)[:, :HEAD_DIM].astype(BF16)
    values[...] = both[:, HEAD_DIM:].astype(BF16)
    for at in range(0, length, STRIP):
        strip, seen = pl.ds(at, STRIP), at + STRIP
        shape = (STRIP, seen)
        allowed = lax.broadcasted_iota(jnp.int32, shape, 1) <= at + lax.broadcasted_iota(
            jnp.int32, shape, 0
        )

        @pl.loop(0, heads, unroll=4)
        def _(head):
            scores = dot_nt(queries[head, strip, :], keys[:seen, :]) * HEAD_DIM ** (-0.5)
            scores = jnp.where(allowed, scores, -1e30)
            exponent = jnp.exp(scores - jnp.max(scores, -1, keepdims=True))
            share = (exponent / jnp.sum(exponent, -1, keepdims=True)).astype(BF16)
            weights[head, strip, :seen] = share
            parts[head, strip, :] = dot(share, values[:seen, :])

    context[...] = jnp.concatenate([parts[head] for head in range(heads)], 1).astype(BF16)
    own_input[...] = rows[:, pl.ds(block_start(core, x, 0), BLOCK)]

    @pl.loop(0, 4)
    def _(step):
        there = wo[pl.ds(block_start(1 - core, x, step), BLOCK), :]
        other[step] = dot_nt(context[...], there).astype(BF16)
        here = wo[pl.ds(block_start(core, x, step), BLOCK), :]
        mine[step] = dot_nt(context[...], here).astype(BF16)


def spread(tall, y, targets):
    for step, target in enumerate(targets):
        there = (y + step) % 4

        @pl.loop(0, 8)
        def _(z):
            row = (((there % 2) * 8 + z) * 2 + there // 2) * 64
            target[z] = tall[pl.ds(pl.multiple_of(row, 64), 64), :]


def pull_kernel(place, kept, moved, kept_there, moved_there, down, client_rows, gain, pulled, own_upstream, turned, whole):
    core, x = place[0], place[1]
    rows, wide = kept.shape
    sides = ((core, (kept, moved)), (1 - core, (kept_there, moved_there)))
    for side, halves in sides:
        for half, piece in enumerate(halves):
            start = pl.multiple_of(side * wide, wide)
            whole[pl.ds(half * rows, rows), pl.ds(start, wide)] = piece[...]
    own_upstream[...] = whole[:, pl.ds(block_start(core, x, 0), BLOCK)]
    pulled[...] = dot_nt(whole[...], down.ready()[...])
    client_rows = client_rows.ready()
    for at in range(0, whole.shape[0], STRIP):
        turned[:, at : at + STRIP] = normalize(client_rows, gain, pl.ds(at, STRIP)).T


def server_kernel(
    place, p0, p1, p2, p3, q0, q1, pulled, gain, gate, up,
    mine, other, normed, grads, gates, ups, gate_grad, up_grad, inverse,
):
    core, x = place[0], place[1]
    pieces = (p0, p1, p2, p3, q0, q1.at[0], q1.at[1], q1.at[2])
    width, length = normed.shape[1], p0.shape[0]
    blocks = [
        pl.ds(block_start(core if index < 4 else 1 - core, x, 4 - index % 4), BLOCK)
        for index in range(8)
    ]

    def strips(step):
        @pl.loop(0, length // STRIP)
        def _(at):
            step(pl.ds(pl.multiple_of(at * STRIP, STRIP), STRIP))

    def normalize(strip):
        squares = jnp.zeros((STRIP, 1), F32)
        for piece in pieces:
            rows_float = piece[strip, :].astype(F32)
            squares = squares + jnp.sum(rows_float * rows_float, -1, keepdims=True)
        inv_rms = lax.rsqrt(squares / width + 1e-05)
        inverse[strip, :] = inv_rms
        for piece, some in zip(pieces, blocks):
            scaled = piece[strip, :].astype(F32) * inv_rms * gain[:, some].astype(F32)
            normed[strip, some] = scaled.astype(BF16)

    strips(normalize)
    gate = gate.ready()
    gates[...] = dot(normed[...], gate[...])
    up = up.ready()
    ups[...] = dot(normed[...], up[...])

    def through_gate(strip):
        gate_value, pull = gates[strip, :], pulled[strip, :]
        sigmoid_gate = jax.nn.sigmoid(gate_value)
        slope = sigmoid_gate * (1.0 + gate_value * (1.0 - sigmoid_gate))
        gate_grad[strip, :] = (pull * ups[strip, :] * slope).astype(BF16)
        up_grad[strip, :] = (pull * gate_value * sigmoid_gate).astype(BF16)

    strips(through_gate)
    for index, some in enumerate(blocks):
        grads[index] = dot_nt(gate_grad[...], gate[some, :]) + dot_nt(up_grad[...], up[some, :])

    def finish(strip):
        along = jnp.zeros((STRIP, 1), F32)
        for index, (piece, some) in enumerate(zip(pieces, blocks)):
            weighted = grads[index, strip, :] * gain[:, some].astype(F32)
            grads[index, strip, :] = weighted
            along = along + jnp.sum(weighted * piece[strip, :].astype(F32), -1, keepdims=True)
        inv_rms = inverse[strip, :]
        scale = inv_rms * inv_rms * inv_rms * (along / width)
        for index, piece in enumerate(pieces):
            part = inv_rms * grads[index, strip, :] - piece[strip, :].astype(F32) * scale
            step = (4 - index % 4) % 4
            if index < 4:
                mine[step, strip, :] = part.astype(BF16)
            else:
                other[step, strip, :] = part.astype(BF16)

    strips(finish)


def output_kernel(
    place, p0, p1, p2, p3, q0, q1, wo, context, context_grad, t0, t1, t2, t3, arrived, tall
):
    core, x = place[0], place[1]
    pieces = (p0, p1, p2, p3, q0, q1.at[0], q1.at[1], q1.at[2])
    for index, piece in enumerate(pieces):
        side = core if index < 4 else 1 - core
        some = pl.ds(block_start(side, x, 4 - index % 4), BLOCK)
        rows = piece[...]
        arrived[:, some] = rows
        tall[some, :] = dot_tn(rows, context[...]).astype(BF16)
    grads = dot(arrived[...], wo[...]).astype(BF16)
    for head in range(context_grad.shape[0]):
        context_grad[head] = grads[:, head * HEAD_DIM : (head + 1) * HEAD_DIM]
    spread(tall, place[2], (t0, t1, t2, t3))


def attend_back_kernel(
    place, context_grad, turned, queries, keys, values, weights, fine_cos, fine_sin, coarse_cos, coarse_sin,
    t0, t1, t2, t3, joined, tall, query_grad, key_grad, value_grad,
):
    heads, length = queries.shape[0], queries.shape[1]
    cos2, sin2 = expand_tables(fine_cos, fine_sin, coarse_cos, coarse_sin)
    cos4, sin4 = jnp.concatenate([cos2, cos2], 1), jnp.concatenate([sin2, sin2], 1)
    key_grad[...] = jnp.zeros_like(key_grad)
    value_grad[...] = jnp.zeros_like(value_grad)
    for at in range(0, length, STRIP):
        strip, seen = pl.ds(at, STRIP), at + STRIP

        @pl.loop(0, heads, unroll=2)
        def _(head):
            share, grads = weights[head, strip, :seen], context_grad[head, strip, :]
            share_float = share.astype(F32)
            share_grad = dot_nt(grads, values[:seen, :]).astype(BF16).astype(F32)
            level = jnp.sum(share_grad * share_float, -1, keepdims=True)
            score_grad = (share_float * (share_grad - level) * HEAD_DIM ** (-0.5)).astype(BF16)
            query_grad[head, strip, :] = dot(score_grad, keys[:seen, :])
            key_grad[:seen, :] += dot_tn(score_grad, queries[head, strip, :])
            value_grad[:seen, :] += dot_tn(share, grads)

    of_queries = jnp.concatenate([query_grad[head] for head in range(heads)], 1)
    joined[:, :BLOCK] = rotate_back(of_queries.astype(BF16).astype(F32), cos4, sin4).astype(BF16)
    pair = jnp.concatenate([key_grad[...], value_grad[...]], 1).astype(BF16).astype(F32)
    lane = lax.broadcasted_iota(jnp.int32, pair.shape, 1)
    back = jnp.where(lane < HEAD_DIM, rotate_back(pair, cos2, sin2), pair)
    joined[:, BLOCK:] = back.astype(BF16)
    tall[...] = dot(turned[...], joined[...]).astype(BF16)
    spread(tall, place[2], (t0, t1, t2, t3))


def x_shift(value, step):
    size = lax.axis_size("x")
    return lax.ppermute(value, "x", [(i, (i + step) % size) for i in range(size)])


def core_swap(value):
    return lax.ppermute(value, "core", [(0, 1), (1, 0)])


def group_swap(value):
    return lax.ppermute(value, "yh", [(0, 1), (1, 0)])


def y_shift(value, step):
    def place(y):
        return (y % 2) * 2 + y // 2

    return lax.ppermute(value, ("yl", "yh"), [(place(y), place((y + step) % 4)) for y in range(4)])


def over_clients(pieces):
    return lax.all_to_all(pieces, ("yl", "z"), 0, 0, tiled=True)


def pick(pieces, order):
    return pieces.at[order].get(mode="promise_in_bounds")


def added(*terms):
    return sum(term.astype(F32) for term in terms)


def relay_out(rows, order):
    pieces = over_clients(rows.reshape(16, -1, rows.shape[1]))
    arrived = group_swap(pick(pieces, order[8:]))
    return pieces, arrived


def relay_back(rows, inverse):
    pieces = rows.reshape(16, -1, BLOCK)
    returned = group_swap(pieces[8:])
    ordered = pick(jnp.concatenate([pieces[:8], returned], 0), inverse)
    return over_clients(ordered).reshape(rows.shape)


def share_sum(mine, other, *more):
    arrived = core_swap(other)
    pairs = [added(mine[step], arrived[step]) for step in range(4)]
    parts = [x_shift(pairs[step].astype(BF16), step) for step in (1, 3, 2)]
    return added(pairs[0], *parts, *more).astype(BF16)


def widen_rows(own):
    parts = [x_shift(own, step) for step in (1, 3, 2)]
    rest = [parts[0], parts[2], parts[1]]
    return [own, *rest, core_swap(own), core_swap(jnp.stack(rest))]


def tile_sum(tiles):
    parts = [y_shift(tiles[step], step) for step in (1, 3, 2)]
    summed = added(tiles[0], *parts).astype(BF16)
    pieces = lax.all_to_all(summed, "z", 0, 0, tiled=True)
    return (added(*pieces) / 16).astype(BF16)


def local(
    client_input,
    client_gain,
    query_weight,
    key_weight,
    client_value_weight,
    output_weight,
    server_gain,
    server_gate,
    server_up,
    server_down,
    upstream,
    assignment,
):
    length = client_input.shape[0]
    x, core, group = lax.axis_index("x"), lax.axis_index("core"), lax.axis_index("yh")
    at, y = jnp.arange(3), group * 2 + lax.axis_index("yl")
    place = jnp.where(at == 0, core, jnp.where(at == 1, x, y))
    leaves = (assignment != group).astype(jnp.int32)
    clients = jnp.arange(16)
    before = (clients[:, None] > clients[None, :]) & (leaves[:, None] == leaves[None, :])
    inverse = jnp.sum(before.astype(jnp.int32), 1) + 8 * leaves
    order = jnp.sum(jnp.where(inverse[None, :] == clients[:, None], clients[None, :], 0), 1)
    tables = rotary_tables(length)

    half = 4 * BLOCK
    own_upstream = lax.dynamic_slice_in_dim(upstream, core * half, half, 1)
    piece, stack = ((length, BLOCK), BF16), ((4, length, BLOCK), BF16)
    head = ((length, HEAD_DIM), BF16)
    heads = query_weight.shape[2] // HEAD_DIM
    by_head = ((heads, length, HEAD_DIM), BF16)
    fwd = on_core(
        attend_kernel,
        [stack, stack, piece, by_head, head, head]
        + [((heads, length, length), BF16), piece],
        [pltpu.VMEM((heads, length, HEAD_DIM), F32), pltpu.VMEM(client_input.shape, BF16)],
        limit=60,
    )(
        place, client_input, client_gain, query_weight[0], key_weight[0].T,
        client_value_weight[0].T, output_weight[0], *tables,
    )
    mine, other, (own_input, queries, keys, values, weights, context) = (
        fwd[0], fwd[1], fwd[2:],
    )
    pieces, moved = relay_out(own_upstream, order)
    kept = pick(pieces, order[:8]).reshape(-1, half)
    moved = moved.reshape(-1, half)
    there = (core_swap(kept), core_swap(moved))
    pulled, server_upstream, turned = on_core(
        pull_kernel,
        [((length, server_down.shape[1]), F32), piece, (client_input.shape[::-1], BF16)],
        [pltpu.VMEM(client_input.shape, BF16)],
        late=(4, 5),
        limit=60,
    )(place, kept, moved, *there, server_down[0], client_input, client_gain)
    cut_input = share_sum(mine, other, own_input)
    pieces, moved = relay_out(cut_input, order)
    arranged = lax.dynamic_update_slice_in_dim(pick(pieces, order), moved, 8, 0)
    wide_rows = widen_rows(arranged.reshape(length, BLOCK))
    back = on_core(
        server_kernel,
        [stack, stack],
        [
            pltpu.VMEM(client_input.shape, BF16),
            pltpu.VMEM((8, length, BLOCK), F32),
            pltpu.VMEM((length, server_gate.shape[2]), F32),
            pltpu.VMEM((length, server_gate.shape[2]), F32),
            pltpu.VMEM((length, server_gate.shape[2]), BF16),
            pltpu.VMEM((length, server_gate.shape[2]), BF16),
            pltpu.VMEM((length, 1), F32),
        ],
        late=(8, 9),
        limit=60,
    )(place, *wide_rows, pulled, server_gain, server_gate[0], server_up[0])
    cut_grad = share_sum(back[0], back[1], server_upstream)
    arriving = widen_rows(relay_back(cut_grad, inverse))
    width = client_input.shape[1]
    context_grad, *outs = on_core(
        output_kernel,
        [by_head] + [((8, 64, BLOCK), BF16)] * 4,
        [pltpu.VMEM(client_input.shape, BF16), pltpu.VMEM((width, BLOCK), BF16)],
    )(place, *arriving, output_weight[0], context)
    joined_width = BLOCK + 2 * HEAD_DIM
    tiles = on_core(
        attend_back_kernel,
        [((8, 64, joined_width), BF16)] * 4,
        [
            pltpu.VMEM((length, joined_width), BF16),
            pltpu.VMEM((width, joined_width), BF16),
            pltpu.VMEM((heads, length, HEAD_DIM), F32),
            pltpu.VMEM((length, HEAD_DIM), F32),
            pltpu.VMEM((length, HEAD_DIM), F32),
        ],
    )(place, context_grad, turned, queries, keys, values, weights, *tables)
    output_update = tile_sum(outs)
    total = tile_sum(tiles)
    return (
        total[:, :BLOCK],
        total[:, BLOCK : BLOCK + HEAD_DIM],
        total[:, BLOCK + HEAD_DIM :],
        output_update,
    )


def solution(mesh):
    fine = Mesh(mesh.devices.reshape(2, 8, 4, 2, 2), ("yl", "z", "x", "core", "yh"))
    client, tensor, sdata = ("yl", "z"), ("x", "core"), "yh"
    rows = ("yl", "z", "yh")
    placed = (
        P(rows, None),
        P(client, None),
        P(client, None, tensor),
        P(client, None, tensor),
        P(client, None, tensor),
        P(client, None, tensor),
        P(sdata, None),
        P(sdata, None, tensor),
        P(sdata, None, tensor),
        P(sdata, tensor, None),
        P(rows, None),
        P(),
    )
    return jax.shard_map(
        local,
        mesh=fine,
        in_specs=placed,
        out_specs=(P(rows, tensor), P(rows, tensor), P(rows, tensor), P(rows, tensor)),
        check_vma=False,
    )
```
